32 devices in a mesh: dp: 8 (over z, y), fsdp: 4 (over x, core).
Axes of the slice: x: 2, y: 2, z: 4, core: 2. Of those that a mesh axis runs over, the one named last changes fastest.
Arguments:
- momentum: float32 [2, 6144, 16384], P(None, 'fsdp', 'dp'), may hold values from -160 to 160, as said below
- gradient: bfloat16 [2, 6144, 16384], P(None, 'fsdp', 'dp'), may hold values from -6 to 6
- q_factor: float32 [2, 16384, 256], P(None, 'dp'), may hold values from -6 to 6
Outputs:
- new_momentum: float32 [2, 6144, 16384], P(None, 'fsdp', 'dp')
- update: bfloat16 [2, 6144, 16384], P(None, 'fsdp', 'dp')
- new_q: float32 [2, 16384, 256], P(None, 'dp')
The draws below stay inside these ranges and needn't reach their ends.
Inputs may be any that keep to these rules, and one draw needn't show every extreme that they name: `momentum`: Real-valued entries.
All inputs are finite; a program needn't handle non-finite values.
Results may differ from the reference program's by a relative error of at most 0.001.
Values sent between devices are 32-bit elements; how exact they have to be, the bound alone decides.
A program may use at most 192 MiB of HBM per device.

```python
import jax
import jax.numpy as jnp
from jax import lax

M = 6144
N = 16384
R = 256
E = 2


def draw_momentum(key, part):
    random_key, row_key, col_key = jax.random.split(key, 3)
    row_place = jnp.arange(M, dtype=jnp.float32) / M - 0.5
    col_place = jnp.arange(N, dtype=jnp.float32) / N - 0.5
    random_part = jax.random.truncated_normal(random_key, -5.0, 5.0, (E, M, N), jnp.float32)
    spread = 1.15
    growth = 3.0
    row_scale = jnp.exp(row_place[None, :, None] * jnp.log(growth) + jax.random.uniform(row_key, (E, M, 1), jnp.float32, -spread, spread))
    col_scale = jnp.exp(col_place[None, None, :] * jnp.log(growth) + jax.random.uniform(col_key, (E, 1, N), jnp.float32, -spread, spread))
    return random_part * row_scale * col_scale


def steps_of(own_key, extent, cuts, low, top_value):
    loudness = 1.0
    for axis_at, parts in cuts:
        draws = jax.random.uniform(jax.random.fold_in(jax.random.fold_in(own_key, 6), axis_at), (parts,), jnp.float32, low / len(cuts), top_value / len(cuts))
        loudness = loudness * jnp.repeat(jnp.exp(draws), extent[axis_at] // parts).reshape((-1,) + (1,) * (len(extent) - 1 - axis_at))
    return loudness


def gaussian(key, shape, scale, limit, cuts=(), kind=jnp.bfloat16):
    factor_of = steps_of(key, shape, cuts, -0.22, 0.18) if cuts else 1.0
    drawn = jax.random.normal(key, shape, jnp.float32) * scale * factor_of
    return jnp.minimum(jnp.maximum(drawn, -limit), limit).astype(kind)


def setup_inputs(seed: int = 0) -> dict:
    arg_keys = jax.random.split(jax.random.key(seed), 4)
    momentum = draw_momentum(jax.random.fold_in(arg_keys[3], 71), 0)
    gradient = gaussian(arg_keys[1], (E, M, N), 1.0, 6.0, ((1, 4), (2, 8)))
    q_factor = gaussian(arg_keys[2], (E, N, R), 1.0, 6.0, ((1, 8),), jnp.float32)
    return {"momentum": momentum, "gradient": gradient, "q_factor": q_factor}


ema_decay = 0.75
epsilon = 1e-06

def one_matrix(inputs):
    moment_part, grad_part, q_part = inputs
    buffer = moment_part + grad_part.astype(jnp.float32)
    left = jnp.dot(buffer, q_part, precision=lax.Precision.HIGHEST)
    gram_matrix = jnp.dot(left.T, left, precision=lax.Precision.HIGHEST)
    lower_factor = jnp.linalg.cholesky(gram_matrix)
    orthonormal = lax.linalg.triangular_solve(lower_factor, left, left_side=False, lower=True, transpose_a=True)
    right_factor = jnp.dot(buffer.T, orthonormal, precision=lax.Precision.HIGHEST)
    new_moment = buffer - (1.0 - ema_decay) * jnp.dot(orthonormal, right_factor.T, precision=lax.Precision.HIGHEST)
    mean_square = lax.optimization_barrier(jnp.mean(right_factor * right_factor, axis=0))
    next_q = right_factor * lax.rsqrt(mean_square + epsilon)[None, :]
    direction = jnp.dot(orthonormal, next_q.T, precision=lax.Precision.HIGHEST) * jnp.sqrt(jnp.float32(M) / jnp.float32(R))
    return (new_moment, direction.astype(jnp.bfloat16), next_q)

def reference(momentum, gradient, q_factor):
    new_momentum, update, new_q = lax.map(one_matrix, (momentum, gradient, q_factor))
    return (new_momentum, update, new_q)
```

```python
import functools

import jax
import jax.numpy as jnp
from jax import lax
from jax.experimental import pallas as pl
from jax.experimental.pallas import tpu as pltpu
from jax.sharding import PartitionSpec as P

ema_decay = 0.75
epsilon = 1e-06
BLOCK = 128
FULL = lax.Precision.HIGHEST
THREE = lax.Precision.HIGH
ONE = lax.Precision.DEFAULT


def inverse_factor_kernel(gram_ref, out_ref, work_left, work_right):
    matrices, size, _ = gram_ref.shape
    rows = lax.broadcasted_iota(jnp.int32, (size, 1), 0)
    lanes = lax.broadcasted_iota(jnp.int32, (1, size), 1)
    eye = jnp.where(rows == lanes, 1.0, 0.0).astype(jnp.float32)
    for e in range(matrices):
        work_left[e] = gram_ref[e]
        work_right[e] = eye

    def step(k, carry):
        for e in range(matrices):
            left = work_left[e]
            right = work_right[e]
            row_left = work_left[e, pl.ds(k, 1), :]
            row_right = work_right[e, pl.ds(k, 1), :]
            pivot = jnp.sum(jnp.where(lanes == k, row_left, 0.0), axis=1, keepdims=True)
            inverse = lax.rsqrt(pivot)
            row_left = row_left * inverse
            row_right = row_right * inverse
            column = jnp.sum(jnp.where(lanes == k, left, 0.0), axis=1, keepdims=True)
            column = jnp.where(rows > k, column * inverse, 0.0)
            work_left[e] = left - column * row_left
            work_right[e] = jnp.where(rows == k, row_right, right - column * row_right)
        return carry

    lax.fori_loop(0, size, step, 0)
    for e in range(matrices):
        out_ref[e] = work_right[e]


def inverse_factor(gram):
    matrices, size, _ = gram.shape
    if size > BLOCK:
        half = size // 2
        top = inverse_factor(gram[:, :half, :half])
        low = jnp.einsum("eij,ekj->eik", gram[:, half:, :half], top, precision=FULL)
        rest = gram[:, half:, half:] - jnp.einsum("eij,ekj->eik", low, low, precision=FULL)
        bottom = inverse_factor(rest)
        cross = -jnp.einsum(
            "eij,ejk->eik", bottom, jnp.einsum("eij,ejk->eik", low, top, precision=FULL), precision=FULL
        )
        zero = jnp.zeros_like(cross).swapaxes(1, 2)
        return jnp.concatenate(
            [jnp.concatenate([top, zero], 2), jnp.concatenate([cross, bottom], 2)], 1
        )
    return pl.pallas_call(
        inverse_factor_kernel,
        out_shape=jax.ShapeDtypeStruct(gram.shape, jnp.float32),
        in_specs=[pl.BlockSpec(memory_space=pltpu.VMEM)],
        out_specs=pl.BlockSpec(memory_space=pltpu.VMEM),
        scratch_shapes=[pltpu.VMEM((matrices, size, size), jnp.float32)] * 2,
        cost_estimate=pl.CostEstimate(
            flops=size * size * size * 4 * matrices, bytes_accessed=8 * size * size * matrices, transcendentals=0
        ),
        name="inverse_factor",
    )(gram)


def swap(value, axis, mask):
    size = lax.axis_size(axis)
    return lax.ppermute(value, axis, [(i, i ^ mask) for i in range(size)])


def levels_of(size):
    return [(1, 0) if i == 0 else ((2 << i) - 2, i) for i in range(size.bit_length() - 1)]


def side_of(index, bit):
    if bit == 0:
        return index & 1
    return ((index >> bit) ^ (index >> (bit + 1))) & 1


def keep_half(value, axis, mask, side):
    half = value.shape[0] // 2
    own = lax.dynamic_slice_in_dim(value, side * half, half, 0)
    other = lax.dynamic_slice_in_dim(value, (1 - side) * half, half, 0)
    return own + swap(other, axis, mask)


def both_halves(value, axis, mask, side):
    other = swap(value, axis, mask)
    return jnp.where(
        side == 0, jnp.concatenate([value, other], 0), jnp.concatenate([other, value], 0)
    )


def sum_halving(value, axis, levels):
    index = lax.axis_index(axis)
    for mask, bit in levels:
        value = keep_half(value, axis, mask, side_of(index, bit))
    for mask, bit in reversed(levels):
        value = both_halves(value, axis, mask, side_of(index, bit))
    return value


def sum_doubling(value, axis, levels):
    for mask, _ in levels:
        value = value + swap(value, axis, mask)
    return value


def sum_near_first(value, axis, levels):
    index = lax.axis_index(axis)
    mask, bit = levels[0]
    side = side_of(index, bit)
    value = keep_half(value, axis, mask, side)
    value = sum_doubling(value, axis, levels[1:])
    return both_halves(value, axis, mask, side)


def body(momentum, gradient, q_factor):
    matrices, local_rows, local_cols = momentum.shape
    rank_width = q_factor.shape[2]
    total_rows = local_rows * lax.axis_size("fsdp")
    total_cols = local_cols * lax.axis_size("dp")
    dp_levels = levels_of(lax.axis_size("dp"))
    fsdp_levels = levels_of(lax.axis_size("fsdp"))
    buffers = [momentum[e] + gradient[e].astype(jnp.float32) for e in range(matrices)]
    lefts, grams, rights = [], [], []
    for e in range(matrices):
        partial_value = jnp.einsum("cn,nr->cr", buffers[e], q_factor[e], precision=THREE)
        order = dp_levels if e % 2 == 0 else dp_levels[1:2] + dp_levels[:1] + dp_levels[2:]
        left = sum_halving(partial_value, "dp", order)
        gram = jnp.einsum("cr,ck->rk", left, left, precision=FULL)
        lefts.append(left)
        grams.append(sum_doubling(gram, "fsdp", fsdp_levels))
        right_raw = jnp.einsum("cn,cr->nr", buffers[e], left, precision=THREE)
        rights.append(sum_near_first(right_raw, "fsdp", fsdp_levels))
    inverse = inverse_factor(jnp.stack(grams))
    orthos = [jnp.einsum("cr,kr->ck", lefts[e], inverse[e], precision=FULL) for e in range(matrices)]
    factors = [jnp.einsum("nr,kr->nk", rights[e], inverse[e], precision=FULL) for e in range(matrices)]
    squares = jnp.stack([jnp.sum(f * f, axis=0) for f in factors])
    squares = sum_doubling(squares, "dp", dp_levels)
    col_scale = lax.rsqrt(squares / total_cols + epsilon)
    rms = jnp.sqrt(jnp.float32(total_rows) / jnp.float32(rank_width))
    momenta, updates, new_qs = [], [], []
    for e in range(matrices):
        feedback = jnp.einsum("cr,nr->cn", orthos[e], factors[e], precision=ONE)
        momenta.append(buffers[e] - (1.0 - ema_decay) * feedback)
        new_q = factors[e] * col_scale[e][None, :]
        new_qs.append(new_q)
        direction = jnp.einsum("cr,nr->cn", orthos[e] * rms, new_q, precision=THREE)
        updates.append(direction.astype(jnp.bfloat16))
    return (jnp.stack(momenta), jnp.stack(updates), jnp.stack(new_qs))


def solution(mesh):
    placed = (P(None, "fsdp", "dp"), P(None, "fsdp", "dp"), P(None, "dp", None))
    return jax.shard_map(
        body,
        mesh=mesh,
        in_specs=placed,
        out_specs=(P(None, "fsdp", "dp"), P(None, "fsdp", "dp"), P(None, "dp", None)),
        check_vma=False,
    )
```
